32 devices in a mesh: gx: 4 (over z), gy: 2 (over y), gz: 4 (over x, core).
Axes of the slice: x: 2, y: 2, z: 4, core: 2. Of those that a mesh axis runs over, the one named last changes fastest.
Arguments:
- displacement: float32 [3, 64, 64, 1024], P(None, 'gx', 'gy', 'gz'), may hold values from -1.5 to 1.5
- density: float32 [64, 64, 1024], P('gx', 'gy', 'gz'), may hold values from 0.03 to 1
- stiffness: float32 [24, 24], replicated, may hold values from -9 to 9.5, as said below
Outputs:
- filtered: float32 [64, 64, 1024], P('gx', 'gy', 'gz')
- compliance: float32 [], replicated
- volume: float32 [], replicated
The draws below stay inside these ranges and needn't reach their ends.
Inputs may be any that keep to these rules, and one draw needn't show every extreme that they name: `stiffness`: symmetric and positive definite, every eigenvalue at least 0.5.
All inputs are finite; a program needn't handle non-finite values.
Results may differ from the reference program's by a relative error of at most 0.00005.
Values sent between devices are 32-bit elements; how exact they have to be, the bound alone decides.
A program may use at most 64 MiB of HBM per device.

```python
import jax
import jax.numpy as jnp
from jax import lax

NX = 64
NY = 64
NZ = 1024


def draw_density(key, part):
    levels = jax.random.uniform(key, (NX, NY, NZ), jnp.float32, 0.1, 1.0)
    rising = (1.0 + 2.0 * jnp.arange(NX, dtype=jnp.float32) / max(NX - 1, 1)) / 3.0
    return levels * rising[:, None, None]


def draw_stiffness(key, part):
    factors = jax.random.truncated_normal(key, -3.0, 3.0, (24, 24), jnp.float32)
    factors = factors / jnp.sqrt(24.0)
    return jnp.dot(factors, factors.T, precision=lax.Precision.HIGHEST) + 0.5 * jnp.eye(24, dtype=jnp.float32)


def level_of(own_key, dims, cuts, least, top_value):
    def one(axis_at, shards_of):
        steps = jax.random.uniform(jax.random.fold_in(jax.random.fold_in(own_key, 6), axis_at), (shards_of,), jnp.float32, least / len(cuts), top_value / len(cuts))
        return jnp.repeat(jnp.exp(steps), dims[axis_at] // shards_of).reshape((-1,) + (1,) * (len(dims) - axis_at - 1))

    level = one(*cuts[0])
    for cut in cuts[1:]:
        level = level * one(*cut)
    return level


def bell_draw(key, dims, deviation, bound, pieces=(), kind=jnp.bfloat16):
    values = deviation * jax.random.normal(key, dims, jnp.float32)
    if pieces:
        values = values * level_of(key, dims, pieces, -0.22, 0.18)
    return jnp.clip(values, -bound, bound).astype(kind)


def setup_inputs(seed: int = 0) -> dict:
    seeds = jax.random.split(jax.random.key(seed), 4)
    displacement = bell_draw(seeds[0], (3, NX, NY, NZ), 0.25, 1.5, ((1, 4), (2, 2), (3, 4)), jnp.float32)
    density = draw_density(jax.random.fold_in(seeds[3], 71), 0)
    stiffness = draw_stiffness(jax.random.fold_in(seeds[3], 71), 0)
    return {"displacement": displacement, "density": density, "stiffness": stiffness}


VOID_STIFFNESS = 1e-3
KERNEL = (1.0, 2.0, 3.0, 2.0, 1.0)


def smooth(values, along):
    length = values.shape[along] - 4
    summed = None
    for offset in range(5):
        section = lax.slice_in_dim(values, offset, offset + length, axis=along)
        scaled = KERNEL[offset] * section
        summed = scaled if summed is None else summed + scaled
    return summed


def side_sums(first, amount, extent):
    position = first + jnp.arange(amount, dtype=jnp.int32)
    summed = jnp.zeros((amount,), jnp.float32)
    for offset in range(5):
        inside = (position + offset - 2 >= 0) & (position + offset - 2 < extent)
        summed = summed + KERNEL[offset] * inside.astype(jnp.float32)
    return summed


def plane_energy(slab_nodes, stiffness):
    height = slab_nodes.shape[2] - 1
    length = slab_nodes.shape[3] - 1
    corner_rows = jnp.stack([slab_nodes[member, along_x, along_y:along_y + height, along_z:along_z + length].reshape(-1)
                             for member in range(3) for along_x in range(2) for along_y in range(2) for along_z in range(2)])
    product = jnp.dot(stiffness, corner_rows, precision=lax.Precision.HIGHEST, preferred_element_type=jnp.float32)
    return jnp.sum(corner_rows * product, axis=0).reshape(height, length)


def energies(node_field, stiffness, planes):
    def one_plane(plane_index):
        slab_nodes = lax.dynamic_slice_in_dim(node_field, plane_index, 2, 1)
        return plane_energy(slab_nodes, stiffness)
    return lax.map(one_plane, jnp.arange(planes, dtype=jnp.int32))


def reference(displacement, density, stiffness):
    node_field = jnp.pad(displacement, ((0, 0), (0, 1), (0, 1), (0, 1)))
    energy = energies(node_field, stiffness, NX)
    modulus = VOID_STIFFNESS + density * density * density * (1.0 - VOID_STIFFNESS)
    cell_count = float(NX * NY * NZ)
    compliance = jnp.sum(modulus * energy) / cell_count
    volume = jnp.sum(density) / cell_count
    sensitivity = -3.0 * (1.0 - VOID_STIFFNESS) * density * density * energy
    hole_sum = side_sums(0, NX, NX)[:, None, None] * side_sums(0, NY, NY)[None, :, None] * side_sums(0, NZ, NZ)[None, None, :]
    weighted = sensitivity / hole_sum
    padded = jnp.pad(weighted, 2)
    filtered = smooth(smooth(smooth(padded, 0), 1), 2)
    return filtered, compliance, volume
```

```python
import functools

import jax
import jax.numpy as jnp
from jax import lax
from jax.experimental import pallas as pl
from jax.experimental.pallas import tpu as pltpu
from jax.sharding import PartitionSpec as P

VOID = 0.001
H = (1.0, 2.0, 3.0, 2.0, 1.0)
MESH = pl.DeviceIdType.MESH
AXES = ("gx", "gy", "gz")
F32 = jnp.float32
BF16 = jnp.bfloat16
NODE_STEPS = [(a, b, c) for a in (0, 1) for b in (0, 1) for c in (0, 1) if a + b + c]


def iota(shape, dim):
    return lax.broadcasted_iota(jnp.int32, shape, dim)


def line_sum(position, extent):
    total = None
    for d in range(5):
        at = position + (d - 2)
        term = jnp.where((at >= 0) & (at < extent), H[d], 0.0).astype(F32)
        total = term if total is None else total + term
    return total


def band_weights(stiff):
    rows, cols = 192, 256
    pick = jnp.where((iota((rows, 24), 0) >> 3) == iota((rows, 24), 1), 1.0, 0.0).astype(F32)

    def column(shape):
        col = iota(shape, 1)
        a, g, s = col >> 7, (col >> 4) & 7, col & 7
        cm = jnp.where(g == 6, s, g)
        c = jnp.where(cm >= 3, 1, 0)
        m = cm - 3 * c
        valid = (g < 6) | ((g == 6) & (s < 6))
        return 8 * m + 4 * a + c, valid, jnp.where(g == 6, 8, s), (col >> 3) & 1

    total = None
    for b in (0, 1):
        q, valid, _, _ = column((24, cols))
        place = jnp.where((iota((24, cols), 0) == q + 2 * b) & valid, 1.0, 0.0).astype(F32)
        wide = jnp.dot(stiff, place, precision=lax.Precision.HIGHEST, preferred_element_type=F32)
        tall = jnp.dot(pick, wide, precision=lax.Precision.HIGHEST, preferred_element_type=F32)
        _, _, jj, _ = column((rows, cols))
        term = jnp.where(jj - (iota((rows, cols), 0) & 7) == b, tall, 0.0)
        total = term if total is None else total + term
    high = total.astype(BF16).astype(F32)
    _, _, _, lo_col = column((rows, cols))
    low = jnp.where(lo_col == 0, total - high, 0.0)
    return high.astype(BF16), low.astype(BF16)


def kernel(
    sizes, u, rho, stiff, out, comp, vol,
    rx, ry, rxy, rz, ys, zs, field, parts, weights, wx, wy, yslo, yshi, rylo, ryhi,
    zslo, zshi, rzlo, rzhi, sums, nsend, nrecv, fsend, frecv, gsend, grecv,
):
    ni, nj, nk = rho.shape
    n = dict(zip(AXES, sizes))
    me = {axis: lax.axis_index(axis) for axis in AXES}
    down = {axis: me[axis] > 0 for axis in AXES}
    up = {axis: me[axis] < n[axis] - 1 for axis in AXES}

    def moved(step, sign):
        ids, ok = {}, None
        for axis, s in zip(AXES, step):
            if s:
                ids[axis] = me[axis] + sign * s
                flag = up[axis] if sign > 0 else down[axis]
                ok = flag if ok is None else jnp.logical_and(ok, flag)
        return ids, ok

    barrier = pltpu.get_barrier_semaphore()
    for axis in AXES:
        for off in range(1, n[axis]):
            pl.semaphore_signal(
                barrier, inc=1, device_id={axis: lax.rem(me[axis] + off, n[axis])}, device_id_type=MESH
            )
    for step in NODE_STEPS:
        if sum(step) > 1:
            for sign in (1, -1):
                ids, ok = moved(step, sign)

                @pl.when(ok)
                def _():
                    pl.semaphore_signal(barrier, inc=1, device_id=ids, device_id_type=MESH)

    lane = iota((nj, 128), 1)
    for m in range(3):
        for i in range(ni):
            ys[m, i : i + 1, :] = u[m, i, 0:1, :]

    def pack(i, acc):
        for m in range(3):
            at = m * ni + i
            acc = jnp.where(lane == at, pltpu.roll(u[m, i, :, 0:128], at, 1), acc)
        return acc

    zs[...] = lax.fori_loop(0, ni, pack, jnp.zeros((nj, 128), F32))
    high, low = band_weights(stiff[...])
    weights[0:192, :] = high
    weights[192:384, :] = low

    peers = sum(n[axis] - 1 for axis in AXES)
    for step in NODE_STEPS:
        if sum(step) > 1:
            for sign in (1, -1):
                peers = peers + jnp.where(moved(step, sign)[1], 1, 0)
    pl.semaphore_wait(barrier, peers)

    node_copies = []
    for at, step in enumerate(NODE_STEPS):
        a, b, c = step
        if c:
            src, dst = zs, rz.at[a, b]
        elif b:
            src, dst = (ys.at[:, 0:8, :], rxy) if a else (ys, ry)
        else:
            src, dst = u.at[:, 0], rx
        ids, ok = moved(step, -1)
        copy = pltpu.make_async_remote_copy(
            src_ref=src, dst_ref=dst, send_sem=nsend.at[at], recv_sem=nrecv.at[at],
            device_id=ids, device_id_type=MESH,
        )
        node_copies.append((copy, ok, moved(step, 1)[1], dst))

        @pl.when(ok)
        def _():
            copy.start()

    for copy, _, has, dst in node_copies:

        @pl.when(has)
        def _():
            copy.wait_recv()

        @pl.when(jnp.logical_not(has))
        def _():
            dst[...] = jnp.zeros(dst.shape, F32)

    last = iota((nj, nk), 1) == nk - 1
    last8 = iota((8, nk), 1) == nk - 1

    def place(m, to, base, row, col, corner, at):
        field[0, m, to, 0:nj, :] = base
        moved_base = pltpu.roll(base, nk - 1, 1)
        side = pltpu.roll(col, 127 - at, 1)
        field[1, m, to, 0:nj, :] = jnp.where(last, jnp.concatenate([side, side], 1), moved_base)
        row8 = jnp.broadcast_to(row, (8, nk))
        field[0, m, to, nj : nj + 8, :] = row8
        side8 = pltpu.roll(corner, 127 - at, 1)
        field[1, m, to, nj : nj + 8, :] = jnp.where(
            last8, jnp.concatenate([side8, side8], 1), pltpu.roll(row8, nk - 1, 1)
        )

    def split(f):
        hi = f.astype(BF16).astype(F32)
        return jnp.concatenate([hi, f - hi], 0).astype(BF16)

    sub8 = iota((8, nk), 0)

    def divide(to):
        for jt in range(nj // 8):
            edge = jnp.zeros((8, nk), F32)
            for cm in range(6):
                c, m = divmod(cm, 3)
                f = field[c, m, to, 8 * jt : 8 * jt + 8, :]
                parts[jt, pl.ds(pl.multiple_of(to * 128, 128) + 16 * cm, 16), :] = split(f)
                row = field[c, m, to, 8 * jt + 8 : 8 * jt + 9, :]
                edge = jnp.where(sub8 == cm, jnp.broadcast_to(row, (8, nk)), edge)
            parts[jt, pl.ds(pl.multiple_of(to * 128, 128) + 96, 16), :] = split(edge)
            parts[jt, pl.ds(pl.multiple_of(to * 128, 128) + 112, 16), :] = jnp.zeros((16, nk), BF16)

    def own_plane(i, carry):
        for m in range(3):
            place(
                m, i, u[m, i], ry[m, pl.ds(i, 1), :], rz[0, 0], rz[0, 1, 0:8, :], m * ni + i
            )
        divide(i)
        return carry

    lax.fori_loop(0, ni, own_plane, 0)
    for m in range(3):
        place(m, ni, rx[m], rxy[m, 0:1, :], rz[1, 0], rz[1, 1, 0:8, :], m * ni)
    divide(ni)

    inv_yz = 1.0 / (
        line_sum(me["gy"] * nj + iota((nj, nk), 0), n["gy"] * nj)
        * line_sum(me["gz"] * nk + iota((nj, nk), 1), n["gz"] * nk)
    )
    wy[0, 0:nj, :] = inv_yz

    def plane(i, carry):
        c_sum, v_sum = carry
        inv_x = 1.0 / line_sum(jnp.full((8, nk), me["gx"] * ni + i, jnp.int32), n["gx"] * ni)
        for jt in range(nj // 8):
            data = parts[jt, pl.ds(pl.multiple_of(i * 128, 128), 256), :]
            product = jnp.dot(weights[...], data, preferred_element_type=F32)
            energy = None
            for r in range(24):
                m, a, b, c = r >> 3, (r >> 2) & 1, (r >> 1) & 1, r & 1
                v = product[8 * r : 8 * r + 8] + product[192 + 8 * r : 200 + 8 * r]
                term = v * field[c, m, i + a, 8 * jt + b : 8 * jt + b + 8, :]
                energy = term if energy is None else energy + term
            d = rho[i, 8 * jt : 8 * jt + 8, :]
            c_sum = c_sum + (VOID + d * d * d * (1.0 - VOID)) * energy
            v_sum = v_sum + d
            wx[i + 2, 8 * jt : 8 * jt + 8, :] = (
                (-3.0 * (1.0 - VOID)) * d * d * energy * (inv_x * wy[0, 8 * jt : 8 * jt + 8, :])
            )
        return c_sum, v_sum

    zero = jnp.zeros((8, nk), F32)
    carry = lax.fori_loop(
        0, 4, lambda t, s: plane(jnp.where(t < 2, t, ni - 4 + t), s), (zero, zero)
    )

    def face_copies(axis, base, down_src, up_src, from_up, from_down):
        copies = []
        for at, src, dst, sign in ((base, down_src, from_up, -1), (base + 1, up_src, from_down, 1)):
            copy = pltpu.make_async_remote_copy(
                src_ref=src, dst_ref=dst, send_sem=fsend.at[at], recv_sem=frecv.at[at],
                device_id={axis: me[axis] + sign}, device_id_type=MESH,
            )
            sends = down[axis] if sign < 0 else up[axis]
            takes = up[axis] if sign < 0 else down[axis]
            copies.append((copy, sends, takes, dst))

            @pl.when(sends)
            def _():
                copy.start()

        return copies

    def arrive(copies):
        for copy, sends, takes, dst in copies:

            @pl.when(takes)
            def _():
                copy.wait_recv()

            @pl.when(jnp.logical_not(takes))
            def _():
                dst[...] = jnp.zeros(dst.shape, F32)

    def finish(copies):
        for copy, sends, _, _ in copies:

            @pl.when(sends)
            def _():
                copy.wait_send()

    slot = {"gx": 0, "gy": n["gx"], "gz": n["gx"] + n["gy"]}
    first_sem = {"gx": 0, "gy": n["gx"], "gz": n["gx"] + n["gy"]}

    def share(axis, value):
        mine = slot[axis] + me[axis]
        sums[mine] = value
        copies = []
        for off in range(1, n[axis]):
            copy = pltpu.make_async_remote_copy(
                src_ref=sums.at[mine], dst_ref=sums.at[mine],
                send_sem=gsend.at[first_sem[axis] + off], recv_sem=grecv.at[first_sem[axis] + off],
                device_id={axis: lax.rem(me[axis] + off, n[axis])}, device_id_type=MESH,
            )
            copy.start()
            copies.append(copy)
        return copies

    def gather(axis, copies):
        for copy in copies:
            copy.wait()
        total = sums[slot[axis]]
        for at in range(1, n[axis]):
            total = total + sums[slot[axis] + at]
        return total

    x_copies = face_copies(
        "gx", 0, wx.at[2:4], wx.at[ni : ni + 2], wx.at[ni + 2 : ni + 4], wx.at[0:2]
    )
    c_sum, v_sum = lax.fori_loop(4, ni, lambda t, s: plane(t - 2, s), carry)
    partial = jnp.concatenate([c_sum[:, :128] + c_sum[:, 128:], v_sum[:, :128] + v_sum[:, 128:]], 0)
    x_sums = share("gx", partial)
    arrive(x_copies)

    def smooth_x(i, carry):
        s = 3.0 * wx[i + 2] + 2.0 * (wx[i + 1] + wx[i + 3]) + (wx[i] + wx[i + 4])
        wy[i, 8 : 8 + nj, :] = s
        for at in range(2):
            yslo[at, pl.ds(i, 1), :] = s[at : at + 1]
            yshi[at, pl.ds(i, 1), :] = s[nj - 2 + at : nj - 1 + at]
        return carry

    lax.fori_loop(0, ni, smooth_x, 0)
    y_copies = face_copies("gy", 2, yslo, yshi, ryhi, rylo)
    y_sums = share("gy", gather("gx", x_sums))
    arrive(y_copies)

    def smooth_y(i, carry):
        lo, hi = carry
        for at in range(2):
            wy[i, 6 + at : 7 + at, :] = rylo[at, pl.ds(i, 1), :]
            wy[i, 8 + nj + at : 9 + nj + at, :] = ryhi[at, pl.ds(i, 1), :]
        t = (
            3.0 * wy[i, 8 : 8 + nj, :]
            + 2.0 * (wy[i, 7 : 7 + nj, :] + wy[i, 9 : 9 + nj, :])
            + (wy[i, 6 : 6 + nj, :] + wy[i, 10 : 10 + nj, :])
        )
        out[i] = t
        mine = (lane >> 1) == i
        lo = jnp.where(mine, pltpu.roll(t[:, 0:128], 2 * i, 1), lo)
        hi = jnp.where(mine, pltpu.roll(t[:, nk - 128 : nk], lax.rem(2 * i + 2, 128), 1), hi)
        return lo, hi

    none = jnp.zeros((nj, 128), F32)
    lo, hi = lax.fori_loop(0, ni, smooth_y, (none, none))
    zslo[...] = lo
    zshi[...] = hi
    z_copies = face_copies("gz", 4, zslo, zshi, rzhi, rzlo)
    z_sums = share("gz", gather("gy", y_sums))
    arrive(z_copies)

    lanes = iota((nj, nk), 1)

    def twice(x):
        return jnp.concatenate([x, x], 1)

    def smooth_z(i, carry):
        t = out[i]
        left, right = rzlo[...], rzhi[...]
        a1 = jnp.where(lanes < 1, twice(pltpu.roll(left, 127 - 2 * i, 1)), pltpu.roll(t, 1, 1))
        a2 = jnp.where(lanes < 2, twice(pltpu.roll(left, lax.rem(128 - 2 * i, 128), 1)), pltpu.roll(t, 2, 1))
        b1 = jnp.where(lanes >= nk - 1, twice(pltpu.roll(right, 127 - 2 * i, 1)), pltpu.roll(t, nk - 1, 1))
        b2 = jnp.where(lanes >= nk - 2, twice(pltpu.roll(right, 126 - 2 * i, 1)), pltpu.roll(t, nk - 2, 1))
        out[i] = 3.0 * t + 2.0 * (a1 + b1) + (a2 + b2)
        return carry

    lax.fori_loop(0, ni, smooth_z, 0)
    total = gather("gz", z_sums)
    cells = float(ni * nj * nk * n["gx"] * n["gy"] * n["gz"])
    comp[0, 0] = jnp.sum(total[0:8]) / cells
    vol[0, 0] = jnp.sum(total[8:16]) / cells
    finish(x_copies)
    finish(y_copies)
    finish(z_copies)
    for copy, ok, _, _ in node_copies:

        @pl.when(ok)
        def _():
            copy.wait_send()


def on_device(sizes, displacement, density, stiffness):
    ni, nj, nk = density.shape
    vmem = pl.BlockSpec(memory_space=pltpu.VMEM)
    smem = pl.BlockSpec(memory_space=pltpu.SMEM)
    members = sum(sizes)
    filtered, comp, vol = pl.pallas_call(
        functools.partial(kernel, sizes),
        out_shape=(
            jax.ShapeDtypeStruct((ni, nj, nk), F32),
            jax.ShapeDtypeStruct((1, 1), F32),
            jax.ShapeDtypeStruct((1, 1), F32),
        ),
        in_specs=[vmem] * 3,
        out_specs=(vmem, smem, smem),
        scratch_shapes=[
            pltpu.VMEM((3, nj, nk), F32),
            pltpu.VMEM((3, ni, nk), F32),
            pltpu.VMEM((3, 8, nk), F32),
            pltpu.VMEM((2, 2, nj, 128), F32),
            pltpu.VMEM((3, ni, nk), F32),
            pltpu.VMEM((nj, 128), F32),
            pltpu.VMEM((2, 3, ni + 1, nj + 8, nk), F32),
            pltpu.VMEM((nj // 8, (ni + 1) * 128, nk), BF16),
            pltpu.VMEM((384, 256), BF16),
            pltpu.VMEM((ni + 4, nj, nk), F32),
            pltpu.VMEM((ni, nj + 16, nk), F32),
            pltpu.VMEM((2, ni, nk), F32),
            pltpu.VMEM((2, ni, nk), F32),
            pltpu.VMEM((2, ni, nk), F32),
            pltpu.VMEM((2, ni, nk), F32),
            pltpu.VMEM((nj, 128), F32),
            pltpu.VMEM((nj, 128), F32),
            pltpu.VMEM((nj, 128), F32),
            pltpu.VMEM((nj, 128), F32),
            pltpu.VMEM((members, 16, 128), F32),
            pltpu.SemaphoreType.DMA((7,)),
            pltpu.SemaphoreType.DMA((7,)),
            pltpu.SemaphoreType.DMA((6,)),
            pltpu.SemaphoreType.DMA((6,)),
            pltpu.SemaphoreType.DMA((members,)),
            pltpu.SemaphoreType.DMA((members,)),
        ],
        compiler_params=pltpu.CompilerParams(
            collective_id=0, has_side_effects=True, vmem_limit_bytes=60 * 1024 * 1024
        ),
    )(displacement, density, stiffness)
    return filtered, comp.reshape(()), vol.reshape(())


def solution(mesh):
    sizes = tuple(mesh.shape[axis] for axis in AXES)
    return jax.shard_map(
        functools.partial(on_device, sizes),
        mesh=mesh,
        in_specs=(P(None, "gx", "gy", "gz"), P("gx", "gy", "gz"), P()),
        out_specs=(P("gx", "gy", "gz"), P(), P()),
        check_vma=False,
    )
```

```python
import functools

import jax
import jax.numpy as jnp
from jax import lax
from jax.experimental import pallas as pl
from jax.experimental.pallas import tpu as pltpu
from jax.sharding import PartitionSpec as P

VOID = 0.001
H = (1.0, 2.0, 3.0, 2.0, 1.0)
MESH = pl.DeviceIdType.MESH
AXES = ("gx", "gy", "gz")
F32 = jnp.float32
BF16 = jnp.bfloat16
NODE_STEPS = [(a, b, c) for a in (0, 1) for b in (0, 1) for c in (0, 1) if a + b + c]
SIDE_STEPS = [(b, c) for b in (-1, 0, 1) for c in (-1, 0, 1) if b or c]


def iota(shape, dim):
    return lax.broadcasted_iota(jnp.int32, shape, dim)


def line_sum(position, extent):
    total = None
    for d in range(5):
        at = position + (d - 2)
        term = jnp.where((at >= 0) & (at < extent), H[d], 0.0).astype(F32)
        total = term if total is None else total + term
    return total


def band_weights(stiff):
    rows, cols = 192, 256
    pick = jnp.where((iota((rows, 24), 0) >> 3) == iota((rows, 24), 1), 1.0, 0.0).astype(F32)

    def column(shape):
        col = iota(shape, 1)
        a, g, s = col >> 7, (col >> 4) & 7, col & 7
        cm = jnp.where(g == 6, s, g)
        c = jnp.where(cm >= 3, 1, 0)
        m = cm - 3 * c
        valid = (g < 6) | ((g == 6) & (s < 6))
        return 8 * m + 4 * a + c, valid, jnp.where(g == 6, 8, s), (col >> 3) & 1

    total = None
    for b in (0, 1):
        q, valid, _, _ = column((24, cols))
        place = jnp.where((iota((24, cols), 0) == q + 2 * b) & valid, 1.0, 0.0).astype(F32)
        wide = jnp.dot(stiff, place, precision=lax.Precision.HIGHEST, preferred_element_type=F32)
        tall = jnp.dot(pick, wide, precision=lax.Precision.HIGHEST, preferred_element_type=F32)
        _, _, jj, _ = column((rows, cols))
        term = jnp.where(jj - (iota((rows, cols), 0) & 7) == b, tall, 0.0)
        total = term if total is None else total + term
    high = total.astype(BF16).astype(F32)
    _, _, _, lo_col = column((rows, cols))
    low = jnp.where(lo_col == 0, total - high, 0.0)
    return high.astype(BF16), low.astype(BF16)


def kernel(
    sizes, u_hbm, rho_hbm, stiff_hbm, out, packs, totals,
    u, rho, stiff, rx, ry, rxy, rz, ys, zs, field, parts, weights, wx, wy,
    yslo, yshi, rylo, ryhi, zslo, zshi, rzz, sums, insem, nsend, nrecv, fsend, frecv, gsend, grecv,
):
    ni, nj, nk = rho.shape
    n = dict(zip(AXES, sizes))
    me = {axis: lax.axis_index(axis) for axis in AXES}
    ny, nz = n["gy"], n["gz"]
    down = {axis: me[axis] > 0 for axis in AXES}
    up = {axis: me[axis] < n[axis] - 1 for axis in AXES}

    loads = []
    for at, (src, dst) in enumerate(((stiff_hbm, stiff), (u_hbm, u), (rho_hbm, rho))):
        copy = pltpu.make_async_copy(src, dst, insem.at[at])
        copy.start()
        loads.append(copy)

    def hop(step):
        ids, ok = {}, None
        for axis, s in zip(AXES, step):
            if s:
                ids[axis] = me[axis] + s
                flag = up[axis] if s > 0 else down[axis]
                ok = flag if ok is None else jnp.logical_and(ok, flag)
        return ids, ok

    def minus(step):
        return tuple(-s for s in step)

    line = [{"gx": lax.rem(me["gx"] + off, n["gx"])} for off in range(1, n["gx"])]
    sheet = [
        {"gy": lax.rem(me["gy"] + off // nz, ny), "gz": lax.rem(me["gz"] + off % nz, nz)}
        for off in range(1, ny * nz)
    ]
    barrier = pltpu.get_barrier_semaphore()
    for ids in line + sheet:
        pl.semaphore_signal(barrier, inc=1, device_id=ids, device_id_type=MESH)
    peers = len(line) + len(sheet)
    for step in NODE_STEPS:
        if step[0] and sum(step) > 1:
            for way in (step, minus(step)):
                ids, ok = hop(way)
                peers = peers + jnp.where(ok, 1, 0)

                @pl.when(ok)
                def _():
                    pl.semaphore_signal(barrier, inc=1, device_id=ids, device_id_type=MESH)

    loads[0].wait()
    high, low = band_weights(stiff[...])
    weights[0:192, :] = high
    weights[192:384, :] = low

    loads[1].wait()
    lane = iota((nj, 128), 1)
    for m in range(3):
        for i in range(ni):
            ys[m, i : i + 1, :] = u[m, i, 0:1, :]

    def pack(i, acc):
        for m in range(3):
            at = m * ni + i
            acc = jnp.where(lane == at, pltpu.roll(u[m, i, :, 0:128], at, 1), acc)
        return acc

    zs[...] = lax.fori_loop(0, ni, pack, jnp.zeros((nj, 128), F32))
    pl.semaphore_wait(barrier, peers)

    def swap(copies, src, dst, send_sem, recv_sem, step):
        ids, sends = hop(step)
        copy = pltpu.make_async_remote_copy(
            src_ref=src, dst_ref=dst, send_sem=send_sem, recv_sem=recv_sem,
            device_id=ids, device_id_type=MESH,
        )
        copies.append((copy, sends, hop(minus(step))[1], dst))

        @pl.when(sends)
        def _():
            copy.start()

    def arrive(copies):
        for copy, _, takes, dst in copies:

            @pl.when(takes)
            def _():
                copy.wait_recv()

            @pl.when(jnp.logical_not(takes))
            def _():
                dst[...] = jnp.zeros(dst.shape, F32)

    def finish(copies):
        for copy, sends, _, _ in copies:

            @pl.when(sends)
            def _():
                copy.wait_send()

    near, far = [], []
    for at, step in enumerate(NODE_STEPS):
        a, b, c = step
        if c:
            src, dst = zs, rz.at[a, b]
        elif b:
            src, dst = (ys.at[:, 0:8, :], rxy) if a else (ys, ry)
        else:
            src, dst = u.at[:, 0], rx
        swap(far if a else near, src, dst, nsend.at[at], nrecv.at[at], minus(step))

    last = iota((nj, nk), 1) == nk - 1
    last8 = iota((8, nk), 1) == nk - 1
    sub8 = iota((8, nk), 0)

    def split(f):
        hi = f.astype(BF16).astype(F32)
        return jnp.concatenate([hi, f - hi], 0).astype(BF16)

    def put(jt, to, at, f):
        parts[jt, pl.ds(pl.multiple_of(to * 128, 128) + at, 16), :] = split(f)

    def first_half(m, to, base):
        field[0, m, to, 0:nj, :] = base
        for jt in range(nj // 8):
            put(jt, to, 16 * m, base[8 * jt : 8 * jt + 8])

    def second_half(m, to, base, row, col, corner, at):
        side = pltpu.roll(col, 127 - at, 1)
        moved = jnp.where(last, jnp.concatenate([side, side], 1), pltpu.roll(base, nk - 1, 1))
        field[1, m, to, 0:nj, :] = moved
        for jt in range(nj // 8):
            put(jt, to, 48 + 16 * m, moved[8 * jt : 8 * jt + 8])
        row8 = jnp.broadcast_to(row, (8, nk))
        field[0, m, to, nj : nj + 8, :] = row8
        side8 = pltpu.roll(corner, 127 - at, 1)
        field[1, m, to, nj : nj + 8, :] = jnp.where(
            last8, jnp.concatenate([side8, side8], 1), pltpu.roll(row8, nk - 1, 1)
        )

    def edges(to):
        for jt in range(nj // 8):
            edge = jnp.zeros((8, nk), F32)
            for cm in range(6):
                c, m = divmod(cm, 3)
                row = field[c, m, to, 8 * jt + 8 : 8 * jt + 9, :]
                edge = jnp.where(sub8 == cm, jnp.broadcast_to(row, (8, nk)), edge)
            put(jt, to, 96, edge)

    def own_first(i, carry):
        for m in range(3):
            first_half(m, i, u[m, i])
        for jt in range(nj // 8):
            parts[jt, pl.ds(pl.multiple_of(i * 128, 128) + 112, 16), :] = jnp.zeros((16, nk), BF16)
        return carry

    def own_second(i, carry):
        for m in range(3):
            second_half(
                m, i, u[m, i], ry[m, pl.ds(i, 1), :], rz[0, 0], rz[0, 1, 0:8, :], m * ni + i
            )
        edges(i)
        return carry

    lax.fori_loop(0, ni, own_first, 0)
    for jt in range(nj // 8):
        parts[jt, ni * 128 + 112 : ni * 128 + 128, :] = jnp.zeros((16, nk), BF16)
    loads[2].wait()
    wy[0, 0:nj, :] = 1.0 / (
        line_sum(me["gy"] * nj + iota((nj, nk), 0), ny * nj)
        * line_sum(me["gz"] * nk + iota((nj, nk), 1), nz * nk)
    )
    arrive(near)
    lax.fori_loop(0, ni, own_second, 0)
    arrive(far)
    for m in range(3):
        first_half(m, ni, rx[m])
        second_half(m, ni, rx[m], rxy[m, 0:1, :], rz[1, 0], rz[1, 1, 0:8, :], m * ni)
    edges(ni)

    def plane(i, carry):
        c_sum, v_sum = carry
        inv_x = 1.0 / line_sum(jnp.full((8, nk), me["gx"] * ni + i, jnp.int32), n["gx"] * ni)
        for jt in range(nj // 8):
            data = parts[jt, pl.ds(pl.multiple_of(i * 128, 128), 256), :]
            product = jnp.dot(weights[...], data, preferred_element_type=F32)
            energy = None
            for r in range(24):
                m, a, b, c = r >> 3, (r >> 2) & 1, (r >> 1) & 1, r & 1
                v = product[8 * r : 8 * r + 8] + product[192 + 8 * r : 200 + 8 * r]
                term = v * field[c, m, i + a, 8 * jt + b : 8 * jt + b + 8, :]
                energy = term if energy is None else energy + term
            d = rho[i, 8 * jt : 8 * jt + 8, :]
            c_sum = c_sum + (VOID + d * d * d * (1.0 - VOID)) * energy
            v_sum = v_sum + d
            wx[i + 2, 8 * jt : 8 * jt + 8, :] = (
                (-3.0 * (1.0 - VOID)) * d * d * energy * (inv_x * wy[0, 8 * jt : 8 * jt + 8, :])
            )
        return c_sum, v_sum

    zero = jnp.zeros((8, nk), F32)
    carry = lax.fori_loop(
        0, 4, lambda t, s: plane(jnp.where(t < 2, t, ni - 4 + t), s), (zero, zero)
    )
    x_copies = []
    swap(x_copies, wx.at[2:4], wx.at[ni + 2 : ni + 4], fsend.at[8], frecv.at[8], (-1, 0, 0))
    swap(x_copies, wx.at[ni : ni + 2], wx.at[0:2], fsend.at[9], frecv.at[9], (1, 0, 0))
    c_sum, v_sum = lax.fori_loop(4, ni, lambda t, s: plane(t - 2, s), carry)

    def share(base, mine, value, group):
        sums[base + mine] = value
        copies = []
        for off, ids in enumerate(group):
            copy = pltpu.make_async_remote_copy(
                src_ref=sums.at[base + mine], dst_ref=sums.at[base + mine],
                send_sem=gsend.at[base + off], recv_sem=grecv.at[base + off],
                device_id=ids, device_id_type=MESH,
            )
            copy.start()
            copies.append(copy)
        return copies

    def gather(base, copies):
        for copy in copies:
            copy.wait()
        total = sums[base]
        for at in range(1, len(copies) + 1):
            total = total + sums[base + at]
        return total

    partial = jnp.concatenate([c_sum[:, :128] + c_sum[:, 128:], v_sum[:, :128] + v_sum[:, 128:]], 0)
    x_sums = share(0, me["gx"], partial, line)
    arrive(x_copies)

    def smooth_x(i, carry):
        lo, hi = carry
        s = 3.0 * wx[i + 2] + 2.0 * (wx[i + 1] + wx[i + 3]) + (wx[i] + wx[i + 4])
        wy[i, 8 : 8 + nj, :] = s
        for at in range(2):
            yslo[at, pl.ds(i, 1), :] = s[at : at + 1]
            yshi[at, pl.ds(i, 1), :] = s[nj - 2 + at : nj - 1 + at]
        mine = (lane >> 1) == i
        lo = jnp.where(mine, pltpu.roll(s[:, 0:128], 2 * i, 1), lo)
        hi = jnp.where(mine, pltpu.roll(s[:, nk - 128 : nk], lax.rem(2 * i + 2, 128), 1), hi)
        return lo, hi

    none = jnp.zeros((nj, 128), F32)
    lo, hi = lax.fori_loop(0, ni, smooth_x, (none, none))
    zslo[...] = lo
    zshi[...] = hi
    side_copies = []
    for at, (b, c) in enumerate(SIDE_STEPS):
        if c:
            rows = (slice(nj - 8, nj), slice(0, nj), slice(0, 8))[1 - b]
            to = (slice(0, 8), slice(8, 8 + nj), slice(8 + nj, 16 + nj))[1 - b]
            src = (zslo if c < 0 else zshi).at[rows]
            dst = rzz.at[1 if c < 0 else 0, to]
        else:
            src, dst = (yslo, ryhi) if b < 0 else (yshi, rylo)
        swap(side_copies, src, dst, fsend.at[at], frecv.at[at], (0, b, c))
    all_sums = share(n["gx"], me["gy"] * nz + me["gz"], gather(0, x_sums), sheet)
    arrive(side_copies)

    def smooth_rows(ref, at):
        return (
            3.0 * ref[at, 8 : 8 + nj, :]
            + 2.0 * (ref[at, 7 : 7 + nj, :] + ref[at, 9 : 9 + nj, :])
            + (ref[at, 6 : 6 + nj, :] + ref[at, 10 : 10 + nj, :])
        )

    for side in range(2):
        packs[side] = smooth_rows(rzz, side)

    def smooth_y(i, carry):
        for at in range(2):
            wy[i, 6 + at : 7 + at, :] = rylo[at, pl.ds(i, 1), :]
            wy[i, 8 + nj + at : 9 + nj + at, :] = ryhi[at, pl.ds(i, 1), :]
        out[i] = smooth_rows(wy, i)
        return carry

    lax.fori_loop(0, ni, smooth_y, 0)
    totals[...] = gather(n["gx"], all_sums)
    for copies in (near, far, x_copies, side_copies):
        finish(copies)


def last_pass(cells, field, packs, totals, out, comp, vol):
    ni, nj, nk = field.shape
    comp[0, 0] = jnp.sum(totals[0:8]) / cells
    vol[0, 0] = jnp.sum(totals[8:16]) / cells
    lanes = iota((nj, nk), 1)

    def twice(x):
        return jnp.concatenate([x, x], 1)

    def smooth_z(i, carry):
        t = field[i]
        left, right = packs[0], packs[1]
        a1 = jnp.where(lanes < 1, twice(pltpu.roll(left, 127 - 2 * i, 1)), pltpu.roll(t, 1, 1))
        a2 = jnp.where(lanes < 2, twice(pltpu.roll(left, lax.rem(128 - 2 * i, 128), 1)), pltpu.roll(t, 2, 1))
        b1 = jnp.where(lanes >= nk - 1, twice(pltpu.roll(right, 127 - 2 * i, 1)), pltpu.roll(t, nk - 1, 1))
        b2 = jnp.where(lanes >= nk - 2, twice(pltpu.roll(right, 126 - 2 * i, 1)), pltpu.roll(t, nk - 2, 1))
        out[i] = 3.0 * t + 2.0 * (a1 + b1) + (a2 + b2)
        return carry

    lax.fori_loop(0, ni, smooth_z, 0)


def on_device(sizes, displacement, density, stiffness):
    ni, nj, nk = density.shape
    vmem = pl.BlockSpec(memory_space=pltpu.VMEM)
    smem = pl.BlockSpec(memory_space=pltpu.SMEM)
    hbm = pl.BlockSpec(memory_space=pltpu.HBM)
    members = sizes[0] + sizes[1] * sizes[2]
    scratch = [
        displacement.shape, density.shape, stiffness.shape,
        (3, nj, nk), (3, ni, nk), (3, 8, nk), (2, 2, nj, 128), (3, ni, nk), (nj, 128),
        (2, 3, ni + 1, nj + 8, nk),
    ]
    later = [
        (ni + 4, nj, nk), (ni, nj + 16, nk),
        (2, ni, nk), (2, ni, nk), (2, ni, nk), (2, ni, nk),
        (nj, 128), (nj, 128), (2, nj + 16, 128), (members, 16, 128),
    ]
    field, packs, totals = pl.pallas_call(
        functools.partial(kernel, sizes),
        out_shape=(
            jax.ShapeDtypeStruct((ni, nj, nk), F32),
            jax.ShapeDtypeStruct((2, nj, 128), F32),
            jax.ShapeDtypeStruct((16, 128), F32),
        ),
        in_specs=[hbm] * 3,
        out_specs=(vmem, vmem, vmem),
        scratch_shapes=[pltpu.VMEM(shape, F32) for shape in scratch]
        + [pltpu.VMEM((nj // 8, (ni + 1) * 128, nk), BF16), pltpu.VMEM((384, 256), BF16)]
        + [pltpu.VMEM(shape, F32) for shape in later]
        + [pltpu.SemaphoreType.DMA((count,)) for count in (3, 7, 7, 10, 10, members, members)],
        compiler_params=pltpu.CompilerParams(
            collective_id=0, has_side_effects=True, vmem_limit_bytes=24 * 1024 * 1024
        ),
    )(displacement, density, stiffness)
    cells = float(ni * nj * nk * sizes[0] * sizes[1] * sizes[2])
    filtered, comp, vol = pl.pallas_call(
        functools.partial(last_pass, cells),
        out_shape=(
            jax.ShapeDtypeStruct((ni, nj, nk), F32),
            jax.ShapeDtypeStruct((1, 1), F32),
            jax.ShapeDtypeStruct((1, 1), F32),
        ),
        in_specs=[vmem] * 3,
        out_specs=(vmem, smem, smem),
        compiler_params=pltpu.CompilerParams(vmem_limit_bytes=24 * 1024 * 1024),
    )(field, packs, totals)
    return filtered, comp.reshape(()), vol.reshape(())


def solution(mesh):
    sizes = tuple(mesh.shape[axis] for axis in AXES)
    return jax.shard_map(
        functools.partial(on_device, sizes),
        mesh=mesh,
        in_specs=(P(None, "gx", "gy", "gz"), P("gx", "gy", "gz"), P()),
        out_specs=(P("gx", "gy", "gz"), P(), P()),
        check_vma=False,
    )
```

```python
import functools

import jax
import jax.numpy as jnp
from jax import lax
from jax.experimental import pallas as pl
from jax.experimental.pallas import tpu as pltpu
from jax.sharding import PartitionSpec as P

VOID = 0.001
H = (1.0, 2.0, 3.0, 2.0, 1.0)
MESH = pl.DeviceIdType.MESH
AXES = ("gx", "gy", "gz")
F32 = jnp.float32
BF16 = jnp.bfloat16
NODE_STEPS = [(a, b, c) for a in (0, 1) for b in (0, 1) for c in (0, 1) if a + b + c]
SIDE_STEPS = [(b, c) for b in (-1, 0, 1) for c in (-1, 0, 1) if b or c]


def iota(shape, dim):
    return lax.broadcasted_iota(jnp.int32, shape, dim)


def line_sum(position, extent):
    total = None
    for d in range(5):
        at = position + (d - 2)
        term = jnp.where((at >= 0) & (at < extent), H[d], 0.0).astype(F32)
        total = term if total is None else total + term
    return total


def band_weights(stiff):
    rows, cols = 192, 256
    pick = jnp.where((iota((rows, 24), 0) >> 3) == iota((rows, 24), 1), 1.0, 0.0).astype(F32)

    def column(shape):
        col = iota(shape, 1)
        a, g, s = col >> 7, (col >> 4) & 7, col & 7
        cm = jnp.where(g == 6, s, g)
        c = jnp.where(cm >= 3, 1, 0)
        m = cm - 3 * c
        valid = (g < 6) | ((g == 6) & (s < 6))
        return 8 * m + 4 * a + c, valid, jnp.where(g == 6, 8, s), (col >> 3) & 1

    total = None
    for b in (0, 1):
        q, valid, _, _ = column((24, cols))
        place = jnp.where((iota((24, cols), 0) == q + 2 * b) & valid, 1.0, 0.0).astype(F32)
        wide = jnp.dot(stiff, place, precision=lax.Precision.HIGHEST, preferred_element_type=F32)
        tall = jnp.dot(pick, wide, precision=lax.Precision.HIGHEST, preferred_element_type=F32)
        _, _, jj, _ = column((rows, cols))
        term = jnp.where(jj - (iota((rows, cols), 0) & 7) == b, tall, 0.0)
        total = term if total is None else total + term
    high = total.astype(BF16).astype(F32)
    _, _, _, lo_col = column((rows, cols))
    low = jnp.where(lo_col == 0, total - high, 0.0)
    return high.astype(BF16), low.astype(BF16)


def kernel(
    sizes, u_hbm, rho_hbm, stiff_hbm, out, packs, totals,
    u, rho, stiff, rx, ry, rxy, rz, ys, zs, field, parts, weights, wx, wy,
    yslo, yshi, rylo, ryhi, zslo, zshi, rzz, sums, insem, nsend, nrecv, fsend, frecv, gsend, grecv,
):
    ni, nj, nk = rho.shape
    n = dict(zip(AXES, sizes))
    me = {axis: lax.axis_index(axis) for axis in AXES}
    ny, nz = n["gy"], n["gz"]
    down = {axis: me[axis] > 0 for axis in AXES}
    up = {axis: me[axis] < n[axis] - 1 for axis in AXES}

    loads = []
    for at, (src, dst) in enumerate(((stiff_hbm, stiff), (u_hbm, u), (rho_hbm, rho))):
        copy = pltpu.make_async_copy(src, dst, insem.at[at])
        copy.start()
        loads.append(copy)

    def hop(step):
        ids, ok = {}, None
        for axis, s in zip(AXES, step):
            if s:
                ids[axis] = me[axis] + s
                flag = up[axis] if s > 0 else down[axis]
                ok = flag if ok is None else jnp.logical_and(ok, flag)
        return ids, ok

    def minus(step):
        return tuple(-s for s in step)

    line = [{"gx": lax.rem(me["gx"] + off, n["gx"])} for off in range(1, n["gx"])]
    sheet = [
        {"gy": lax.rem(me["gy"] + off // nz, ny), "gz": lax.rem(me["gz"] + off % nz, nz)}
        for off in range(1, ny * nz)
    ]
    barrier = pltpu.get_barrier_semaphore()
    for ids in line + sheet:
        pl.semaphore_signal(barrier, inc=1, device_id=ids, device_id_type=MESH)
    peers = len(line) + len(sheet)
    for step in NODE_STEPS:
        if step[0] and sum(step) > 1:
            for way in (step, minus(step)):
                ids, ok = hop(way)
                peers = peers + jnp.where(ok, 1, 0)

                @pl.when(ok)
                def _():
                    pl.semaphore_signal(barrier, inc=1, device_id=ids, device_id_type=MESH)

    loads[0].wait()
    high, low = band_weights(stiff[...])
    weights[0:192, :] = high
    weights[192:384, :] = low

    loads[1].wait()
    lane = iota((nj, 128), 1)
    for m in range(3):
        for i in range(ni):
            ys[m, i : i + 1, :] = u[m, i, 0:1, :]

    def pack(i, acc):
        for m in range(3):
            at = m * ni + i
            acc = jnp.where(lane == at, pltpu.roll(u[m, i, :, 0:128], at, 1), acc)
        return acc

    zs[...] = lax.fori_loop(0, ni, pack, jnp.zeros((nj, 128), F32))
    pl.semaphore_wait(barrier, peers)

    def swap(copies, src, dst, send_sem, recv_sem, step):
        ids, sends = hop(step)
        copy = pltpu.make_async_remote_copy(
            src_ref=src, dst_ref=dst, send_sem=send_sem, recv_sem=recv_sem,
            device_id=ids, device_id_type=MESH,
        )
        copies.append((copy, sends, hop(minus(step))[1], dst))

        @pl.when(sends)
        def _():
            copy.start()

    def arrive(copies):
        for copy, _, takes, dst in copies:

            @pl.when(takes)
            def _():
                copy.wait_recv()

            @pl.when(jnp.logical_not(takes))
            def _():
                dst[...] = jnp.zeros(dst.shape, F32)

    def finish(copies):
        for copy, sends, _, _ in copies:

            @pl.when(sends)
            def _():
                copy.wait_send()

    near, far = [], []
    for at, step in enumerate(NODE_STEPS):
        a, b, c = step
        if c:
            src, dst = zs, rz.at[a, b]
        elif b:
            src, dst = (ys.at[:, 0:8, :], rxy) if a else (ys, ry)
        else:
            src, dst = u.at[:, 0], rx
        swap(far if a else near, src, dst, nsend.at[at], nrecv.at[at], minus(step))

    last = iota((nj, nk), 1) == nk - 1
    last8 = iota((8, nk), 1) == nk - 1
    sub8 = iota((8, nk), 0)

    def split(f):
        hi = f.astype(BF16).astype(F32)
        return jnp.concatenate([hi, f - hi], 0).astype(BF16)

    def put(jt, to, at, f):
        parts[jt, pl.ds(pl.multiple_of(to * 128, 128) + at, 16), :] = split(f)

    def first_half(m, to, base):
        field[0, m, to, 0:nj, :] = base
        for jt in range(nj // 8):
            put(jt, to, 16 * m, base[8 * jt : 8 * jt + 8])

    def second_half(m, to, base, row, col, corner, at):
        side = pltpu.roll(col, 127 - at, 1)
        moved = jnp.where(last, jnp.concatenate([side, side], 1), pltpu.roll(base, nk - 1, 1))
        field[1, m, to, 0:nj, :] = moved
        for jt in range(nj // 8):
            put(jt, to, 48 + 16 * m, moved[8 * jt : 8 * jt + 8])
        row8 = jnp.broadcast_to(row, (8, nk))
        field[0, m, to, nj : nj + 8, :] = row8
        side8 = pltpu.roll(corner, 127 - at, 1)
        field[1, m, to, nj : nj + 8, :] = jnp.where(
            last8, jnp.concatenate([side8, side8], 1), pltpu.roll(row8, nk - 1, 1)
        )

    def edges(to):
        for jt in range(nj // 8):
            edge = jnp.zeros((8, nk), F32)
            for cm in range(6):
                c, m = divmod(cm, 3)
                row = field[c, m, to, 8 * jt + 8 : 8 * jt + 9, :]
                edge = jnp.where(sub8 == cm, jnp.broadcast_to(row, (8, nk)), edge)
            put(jt, to, 96, edge)

    def own_first(i, carry):
        for m in range(3):
            first_half(m, i, u[m, i])
        for jt in range(nj // 8):
            parts[jt, pl.ds(pl.multiple_of(i * 128, 128) + 112, 16), :] = jnp.zeros((16, nk), BF16)
        return carry

    def own_second(i, carry):
        for m in range(3):
            second_half(
                m, i, u[m, i], ry[m, pl.ds(i, 1), :], rz[0, 0], rz[0, 1, 0:8, :], m * ni + i
            )
        edges(i)
        return carry

    lax.fori_loop(0, ni, own_first, 0)
    for jt in range(nj // 8):
        parts[jt, ni * 128 + 112 : ni * 128 + 128, :] = jnp.zeros((16, nk), BF16)
    loads[2].wait()
    wy[0, 0:nj, :] = 1.0 / (
        line_sum(me["gy"] * nj + iota((nj, nk), 0), ny * nj)
        * line_sum(me["gz"] * nk + iota((nj, nk), 1), nz * nk)
    )
    arrive(near)
    lax.fori_loop(0, ni, own_second, 0)
    arrive(far)
    for m in range(3):
        first_half(m, ni, rx[m])
        second_half(m, ni, rx[m], rxy[m, 0:1, :], rz[1, 0], rz[1, 1, 0:8, :], m * ni)
    edges(ni)

    def plane(i, carry):
        c_sum, v_sum = carry
        inv_x = 1.0 / line_sum(jnp.full((8, nk), me["gx"] * ni + i, jnp.int32), n["gx"] * ni)
        for jt in range(nj // 8):
            data = parts[jt, pl.ds(pl.multiple_of(i * 128, 128), 256), :]
            product = jnp.dot(weights[...], data, preferred_element_type=F32)
            energy = None
            for r in range(24):
                m, a, b, c = r >> 3, (r >> 2) & 1, (r >> 1) & 1, r & 1
                v = product[8 * r : 8 * r + 8] + product[192 + 8 * r : 200 + 8 * r]
                term = v * field[c, m, i + a, 8 * jt + b : 8 * jt + b + 8, :]
                energy = term if energy is None else energy + term
            d = rho[i, 8 * jt : 8 * jt + 8, :]
            c_sum = c_sum + (VOID + d * d * d * (1.0 - VOID)) * energy
            v_sum = v_sum + d
            wx[i + 2, 8 * jt : 8 * jt + 8, :] = (
                (-3.0 * (1.0 - VOID)) * d * d * energy * (inv_x * wy[0, 8 * jt : 8 * jt + 8, :])
            )
        return c_sum, v_sum

    zero = jnp.zeros((8, nk), F32)
    carry = lax.fori_loop(
        0, 4, lambda t, s: plane(jnp.where(t < 2, t, ni - 4 + t), s), (zero, zero)
    )
    x_copies = []
    swap(x_copies, wx.at[2:4], wx.at[ni + 2 : ni + 4], fsend.at[8], frecv.at[8], (-1, 0, 0))
    swap(x_copies, wx.at[ni : ni + 2], wx.at[0:2], fsend.at[9], frecv.at[9], (1, 0, 0))
    c_sum, v_sum = lax.fori_loop(4, ni, lambda t, s: plane(t - 2, s), carry)

    def share(base, mine, value, group):
        sums[base + mine] = value
        copies = []
        for off, ids in enumerate(group):
            copy = pltpu.make_async_remote_copy(
                src_ref=sums.at[base + mine], dst_ref=sums.at[base + mine],
                send_sem=gsend.at[base + off], recv_sem=grecv.at[base + off],
                device_id=ids, device_id_type=MESH,
            )
            copy.start()
            copies.append(copy)
        return copies

    def gather(base, copies):
        for copy in copies:
            copy.wait()
        total = sums[base]
        for at in range(1, len(copies) + 1):
            total = total + sums[base + at]
        return total

    partial = jnp.concatenate([c_sum[:, :128] + c_sum[:, 128:], v_sum[:, :128] + v_sum[:, 128:]], 0)
    x_sums = share(0, me["gx"], partial, line)
    arrive(x_copies)

    def smooth_x(i, carry):
        lo, hi = carry
        s = 3.0 * wx[i + 2] + 2.0 * (wx[i + 1] + wx[i + 3]) + (wx[i] + wx[i + 4])
        wy[i, 8 : 8 + nj, :] = s
        for at in range(2):
            yslo[at, pl.ds(i, 1), :] = s[at : at + 1]
            yshi[at, pl.ds(i, 1), :] = s[nj - 2 + at : nj - 1 + at]
        mine = (lane >> 1) == i
        lo = jnp.where(mine, pltpu.roll(s[:, 0:128], 2 * i, 1), lo)
        hi = jnp.where(mine, pltpu.roll(s[:, nk - 128 : nk], lax.rem(2 * i + 2, 128), 1), hi)
        return lo, hi

    none = jnp.zeros((nj, 128), F32)
    lo, hi = lax.fori_loop(0, ni, smooth_x, (none, none))
    zslo[...] = lo
    zshi[...] = hi
    side_copies = []
    for at, (b, c) in enumerate(SIDE_STEPS):
        if c:
            rows = (slice(nj - 8, nj), slice(0, nj), slice(0, 8))[1 - b]
            to = (slice(0, 8), slice(8, 8 + nj), slice(8 + nj, 16 + nj))[1 - b]
            src = (zslo if c < 0 else zshi).at[rows]
            dst = rzz.at[1 if c < 0 else 0, to]
        else:
            src, dst = (yslo, ryhi) if b < 0 else (yshi, rylo)
        swap(side_copies, src, dst, fsend.at[at], frecv.at[at], (0, b, c))
    all_sums = share(n["gx"], me["gy"] * nz + me["gz"], gather(0, x_sums), sheet)
    arrive(side_copies)

    def smooth_rows(ref, at):
        return (
            3.0 * ref[at, 8 : 8 + nj, :]
            + 2.0 * (ref[at, 7 : 7 + nj, :] + ref[at, 9 : 9 + nj, :])
            + (ref[at, 6 : 6 + nj, :] + ref[at, 10 : 10 + nj, :])
        )

    for side in range(2):
        packs[side] = smooth_rows(rzz, side)

    def smooth_y(i, carry):
        for at in range(2):
            wy[i, 6 + at : 7 + at, :] = rylo[at, pl.ds(i, 1), :]
            wy[i, 8 + nj + at : 9 + nj + at, :] = ryhi[at, pl.ds(i, 1), :]
        out[i] = smooth_rows(wy, i)
        return carry

    lax.fori_loop(0, ni, smooth_y, 0)
    totals[...] = gather(n["gx"], all_sums)
    for copies in (near, far, x_copies, side_copies):
        finish(copies)


def last_pass(cells, field, packs, totals, out, comp, vol):
    ni, nj, nk = field.shape
    comp[0, 0] = jnp.sum(totals[0:8]) / cells
    vol[0, 0] = jnp.sum(totals[8:16]) / cells
    lanes = iota((nj, nk), 1)

    def twice(x):
        return jnp.concatenate([x, x], 1)

    def smooth_z(i, carry):
        t = field[i]
        left, right = packs[0], packs[1]
        a1 = jnp.where(lanes < 1, twice(pltpu.roll(left, 127 - 2 * i, 1)), pltpu.roll(t, 1, 1))
        a2 = jnp.where(lanes < 2, twice(pltpu.roll(left, lax.rem(128 - 2 * i, 128), 1)), pltpu.roll(t, 2, 1))
        b1 = jnp.where(lanes >= nk - 1, twice(pltpu.roll(right, 127 - 2 * i, 1)), pltpu.roll(t, nk - 1, 1))
        b2 = jnp.where(lanes >= nk - 2, twice(pltpu.roll(right, 126 - 2 * i, 1)), pltpu.roll(t, nk - 2, 1))
        out[i] = 3.0 * t + 2.0 * (a1 + b1) + (a2 + b2)
        return carry

    lax.fori_loop(0, ni, smooth_z, 0)


def on_device(sizes, displacement, density, stiffness):
    ni, nj, nk = density.shape
    vmem = pl.BlockSpec(memory_space=pltpu.VMEM)
    smem = pl.BlockSpec(memory_space=pltpu.SMEM)
    hbm = pl.BlockSpec(memory_space=pltpu.HBM)
    members = sizes[0] + sizes[1] * sizes[2]
    scratch = [
        displacement.shape, density.shape, stiffness.shape,
        (3, nj, nk), (3, ni, nk), (3, 8, nk), (2, 2, nj, 128), (3, ni, nk), (nj, 128),
        (2, 3, ni + 1, nj + 8, nk),
    ]
    later = [
        (ni + 4, nj, nk), (ni, nj + 16, nk),
        (2, ni, nk), (2, ni, nk), (2, ni, nk), (2, ni, nk),
        (nj, 128), (nj, 128), (2, nj + 16, 128), (members, 16, 128),
    ]
    field, packs, totals = pl.pallas_call(
        functools.partial(kernel, sizes),
        out_shape=(
            jax.ShapeDtypeStruct((ni, nj, nk), F32),
            jax.ShapeDtypeStruct((2, nj, 128), F32),
            jax.ShapeDtypeStruct((16, 128), F32),
        ),
        in_specs=[hbm] * 3,
        out_specs=(vmem, vmem, vmem),
        scratch_shapes=[pltpu.VMEM(shape, F32) for shape in scratch]
        + [pltpu.VMEM((nj // 8, (ni + 1) * 128, nk), BF16), pltpu.VMEM((384, 256), BF16)]
        + [pltpu.VMEM(shape, F32) for shape in later]
        + [pltpu.SemaphoreType.DMA((count,)) for count in (3, 7, 7, 10, 10, members, members)],
        compiler_params=pltpu.CompilerParams(
            collective_id=0, has_side_effects=True, vmem_limit_bytes=24 * 1024 * 1024
        ),
    )(*(pltpu.with_memory_space_constraint(x, pltpu.HBM) for x in (displacement, density, stiffness)))
    cells = float(ni * nj * nk * sizes[0] * sizes[1] * sizes[2])
    filtered, comp, vol = pl.pallas_call(
        functools.partial(last_pass, cells),
        out_shape=(
            jax.ShapeDtypeStruct((ni, nj, nk), F32),
            jax.ShapeDtypeStruct((1, 1), F32),
            jax.ShapeDtypeStruct((1, 1), F32),
        ),
        in_specs=[vmem] * 3,
        out_specs=(vmem, smem, smem),
        compiler_params=pltpu.CompilerParams(vmem_limit_bytes=24 * 1024 * 1024),
    )(field, packs, totals)
    return filtered, comp.reshape(()), vol.reshape(())


def solution(mesh):
    sizes = tuple(mesh.shape[axis] for axis in AXES)
    return jax.shard_map(
        functools.partial(on_device, sizes),
        mesh=mesh,
        in_specs=(P(None, "gx", "gy", "gz"), P("gx", "gy", "gz"), P()),
        out_specs=(P("gx", "gy", "gz"), P(), P()),
        check_vma=False,
    )
```

```python
import functools

import jax
import jax.numpy as jnp
from jax import lax
from jax.experimental import pallas as pl
from jax.experimental.pallas import tpu as pltpu
from jax.sharding import PartitionSpec as P

VOID = 0.001
H = (1.0, 2.0, 3.0, 2.0, 1.0)
MESH = pl.DeviceIdType.MESH
AXES = ("gx", "gy", "gz")
F32 = jnp.float32
BF16 = jnp.bfloat16
NODE_STEPS = [(a, b, c) for a in (0, 1) for b in (0, 1) for c in (0, 1) if a + b + c]
SIDE_STEPS = [(b, c) for b in (-1, 0, 1) for c in (-1, 0, 1) if b or c]


def iota(shape, dim):
    return lax.broadcasted_iota(jnp.int32, shape, dim)


def line_sum(position, extent):
    total = None
    for d in range(5):
        at = position + (d - 2)
        term = jnp.where((at >= 0) & (at < extent), H[d], 0.0).astype(F32)
        total = term if total is None else total + term
    return total


def band_weights(stiff):
    rows, cols = 192, 256
    pick = jnp.where((iota((rows, 24), 0) >> 3) == iota((rows, 24), 1), 1.0, 0.0).astype(F32)

    def column(shape):
        col = iota(shape, 1)
        a, g, s = col >> 7, (col >> 4) & 7, col & 7
        cm = jnp.where(g == 6, s, g)
        c = jnp.where(cm >= 3, 1, 0)
        m = cm - 3 * c
        valid = (g < 6) | ((g == 6) & (s < 6))
        return 8 * m + 4 * a + c, valid, jnp.where(g == 6, 8, s), (col >> 3) & 1

    total = None
    for b in (0, 1):
        q, valid, _, _ = column((24, cols))
        place = jnp.where((iota((24, cols), 0) == q + 2 * b) & valid, 1.0, 0.0).astype(F32)
        wide = jnp.dot(stiff, place, precision=lax.Precision.HIGHEST, preferred_element_type=F32)
        tall = jnp.dot(pick, wide, precision=lax.Precision.HIGHEST, preferred_element_type=F32)
        _, _, jj, _ = column((rows, cols))
        term = jnp.where(jj - (iota((rows, cols), 0) & 7) == b, tall, 0.0)
        total = term if total is None else total + term
    high = total.astype(BF16).astype(F32)
    _, _, _, lo_col = column((rows, cols))
    low = jnp.where(lo_col == 0, total - high, 0.0)
    return high.astype(BF16), low.astype(BF16)


def kernel(
    sizes, u_hbm, rho_hbm, stiff_hbm, out, packs, totals,
    u, rho, stiff, rx, ry, rxy, rz, ys, yd, zs, field, parts, weights, wx, wy,
    yslo, yshi, rylo, ryhi, zslo, zshi, rzz, sums, insem, nsend, nrecv, fsend, frecv, gsend, grecv,
):
    ni, nj, nk = rho.shape
    n = dict(zip(AXES, sizes))
    me = {axis: lax.axis_index(axis) for axis in AXES}
    ny, nz = n["gy"], n["gz"]
    down = {axis: me[axis] > 0 for axis in AXES}
    up = {axis: me[axis] < n[axis] - 1 for axis in AXES}

    loads = []
    for at, (src, dst) in enumerate(((stiff_hbm, stiff), (u_hbm, u), (rho_hbm, rho))):
        copy = pltpu.make_async_copy(src, dst, insem.at[at])
        copy.start()
        loads.append(copy)

    def hop(step):
        ids, ok = {}, None
        for axis, s in zip(AXES, step):
            if s:
                ids[axis] = me[axis] + s
                flag = up[axis] if s > 0 else down[axis]
                ok = flag if ok is None else jnp.logical_and(ok, flag)
        return ids, ok

    def minus(step):
        return tuple(-s for s in step)

    line = [{"gx": lax.rem(me["gx"] + off, n["gx"])} for off in range(1, n["gx"])]
    sheet = [
        {"gy": lax.rem(me["gy"] + off // nz, ny), "gz": lax.rem(me["gz"] + off % nz, nz)}
        for off in range(1, ny * nz)
    ]
    barrier = pltpu.get_barrier_semaphore()
    for ids in line + sheet:
        pl.semaphore_signal(barrier, inc=1, device_id=ids, device_id_type=MESH)
    peers = len(line) + len(sheet)
    for step in NODE_STEPS:
        if step[0] and sum(step) > 1:
            for way in (step, minus(step)):
                ids, ok = hop(way)
                peers = peers + jnp.where(ok, 1, 0)

                @pl.when(ok)
                def _():
                    pl.semaphore_signal(barrier, inc=1, device_id=ids, device_id_type=MESH)

    pl.semaphore_wait(barrier, peers)

    def swap(copies, src, dst, send_sem, recv_sem, step):
        ids, sends = hop(step)
        copy = pltpu.make_async_remote_copy(
            src_ref=src, dst_ref=dst, send_sem=send_sem, recv_sem=recv_sem,
            device_id=ids, device_id_type=MESH,
        )
        copies.append((copy, sends, hop(minus(step))[1], dst))

        @pl.when(sends)
        def _():
            copy.start()

    def arrive(copies):
        for copy, _, takes, dst in copies:

            @pl.when(takes)
            def _():
                copy.wait_recv()

            @pl.when(jnp.logical_not(takes))
            def _():
                dst[...] = jnp.zeros(dst.shape, F32)

    def finish(copies):
        for copy, sends, _, _ in copies:

            @pl.when(sends)
            def _():
                copy.wait_send()

    beside, below, far = [], [], []

    def node_swap(step):
        a, b, c = step
        at = NODE_STEPS.index(step)
        if c:
            src, dst = (zs.at[0:8], rz.at[a, b, 0:8]) if b else (zs, rz.at[a, b])
        elif b:
            src, dst = (yd, rxy) if a else (ys, ry)
        else:
            src, dst = u_hbm.at[:, 0], rx
        copies = far if a else (below if b else beside)
        swap(copies, src, dst, nsend.at[at], nrecv.at[at], minus(step))

    node_swap((1, 0, 0))
    loads[1].wait()
    lane = iota((nj, 128), 1)
    yd[...] = jnp.zeros(yd.shape, F32)
    for m in range(3):
        for i in range(ni):
            ys[m, i : i + 1, :] = u[m, i, 0:1, :]
        yd[m : m + 1, :] = u[m, 0, 0:1, :]
    node_swap((0, 1, 0))
    node_swap((1, 1, 0))

    def pack(i, acc):
        for m in range(3):
            at = m * ni + i
            acc = jnp.where(lane == at, pltpu.roll(u[m, i, :, 0:128], at, 1), acc)
        return acc

    zs[...] = lax.fori_loop(0, ni, pack, jnp.zeros((nj, 128), F32))
    for step in NODE_STEPS:
        if step[2]:
            node_swap(step)
    loads[0].wait()
    high, low = band_weights(stiff[...])
    weights[0:192, :] = high
    weights[192:384, :] = low

    last = iota((nj, nk), 1) == nk - 1
    last8 = iota((8, nk), 1) == nk - 1
    sub8 = iota((8, nk), 0)

    def split(f):
        hi = f.astype(BF16).astype(F32)
        return jnp.concatenate([hi, f - hi], 0).astype(BF16)

    def put(jt, to, at, f):
        parts[jt, pl.ds(pl.multiple_of(to * 128, 128) + at, 16), :] = split(f)

    def first_half(m, to, base):
        field[0, m, to, 0:nj, :] = base
        for jt in range(nj // 8):
            put(jt, to, 16 * m, base[8 * jt : 8 * jt + 8])

    def second_half(m, to, base, col, at):
        side = pltpu.roll(col, 127 - at, 1)
        moved = jnp.where(last, jnp.concatenate([side, side], 1), pltpu.roll(base, nk - 1, 1))
        field[1, m, to, 0:nj, :] = moved
        for jt in range(nj // 8):
            put(jt, to, 48 + 16 * m, moved[8 * jt : 8 * jt + 8])

    def next_row(m, to, row, corner, at):
        row8 = jnp.broadcast_to(row, (8, nk))
        field[0, m, to, nj : nj + 8, :] = row8
        side8 = pltpu.roll(corner, 127 - at, 1)
        field[1, m, to, nj : nj + 8, :] = jnp.where(
            last8, jnp.concatenate([side8, side8], 1), pltpu.roll(row8, nk - 1, 1)
        )

    def edges(to):
        for jt in range(nj // 8):
            edge = jnp.zeros((8, nk), F32)
            for cm in range(6):
                c, m = divmod(cm, 3)
                row = field[c, m, to, 8 * jt + 8 : 8 * jt + 9, :]
                edge = jnp.where(sub8 == cm, jnp.broadcast_to(row, (8, nk)), edge)
            put(jt, to, 96, edge)

    def own_first(i, carry):
        for m in range(3):
            first_half(m, i, u[m, i])
        for jt in range(nj // 8):
            parts[jt, pl.ds(pl.multiple_of(i * 128, 128) + 112, 16), :] = jnp.zeros((16, nk), BF16)
        return carry

    def own_second(i, carry):
        for m in range(3):
            second_half(m, i, u[m, i], rz[0, 0], m * ni + i)
        return carry

    def own_edges(i, carry):
        for m in range(3):
            next_row(m, i, ry[m, pl.ds(i, 1), :], rz[0, 1, 0:8, :], m * ni + i)
        edges(i)
        return carry

    lax.fori_loop(0, ni, own_first, 0)
    for jt in range(nj // 8):
        parts[jt, ni * 128 + 112 : ni * 128 + 128, :] = jnp.zeros((16, nk), BF16)
    loads[2].wait()
    wy[0, 0:nj, :] = 1.0 / (
        line_sum(me["gy"] * nj + iota((nj, nk), 0), ny * nj)
        * line_sum(me["gz"] * nk + iota((nj, nk), 1), nz * nk)
    )
    arrive(beside)
    lax.fori_loop(0, ni, own_second, 0)
    arrive(below)
    lax.fori_loop(0, ni, own_edges, 0)
    arrive(far)
    for m in range(3):
        first_half(m, ni, rx[m])
        second_half(m, ni, rx[m], rz[1, 0], m * ni)
        next_row(m, ni, rxy[m : m + 1, :], rz[1, 1, 0:8, :], m * ni)
    edges(ni)

    def plane(i, carry):
        c_sum, v_sum = carry
        inv_x = 1.0 / line_sum(jnp.full((8, nk), me["gx"] * ni + i, jnp.int32), n["gx"] * ni)
        for jt in range(nj // 8):
            data = parts[jt, pl.ds(pl.multiple_of(i * 128, 128), 256), :]
            product = jnp.dot(weights[...], data, preferred_element_type=F32)
            energy = None
            for r in range(24):
                m, a, b, c = r >> 3, (r >> 2) & 1, (r >> 1) & 1, r & 1
                v = product[8 * r : 8 * r + 8] + product[192 + 8 * r : 200 + 8 * r]
                term = v * field[c, m, i + a, 8 * jt + b : 8 * jt + b + 8, :]
                energy = term if energy is None else energy + term
            d = rho[i, 8 * jt : 8 * jt + 8, :]
            c_sum = c_sum + (VOID + d * d * d * (1.0 - VOID)) * energy
            v_sum = v_sum + d
            wx[i + 2, 8 * jt : 8 * jt + 8, :] = (
                (-3.0 * (1.0 - VOID)) * d * d * energy * (inv_x * wy[0, 8 * jt : 8 * jt + 8, :])
            )
        return c_sum, v_sum

    zero = jnp.zeros((8, nk), F32)
    carry = lax.fori_loop(
        0, 4, lambda t, s: plane(jnp.where(t < 2, t, ni - 4 + t), s), (zero, zero)
    )
    x_copies = []
    swap(x_copies, wx.at[2:4], wx.at[ni + 2 : ni + 4], fsend.at[8], frecv.at[8], (-1, 0, 0))
    swap(x_copies, wx.at[ni : ni + 2], wx.at[0:2], fsend.at[9], frecv.at[9], (1, 0, 0))
    c_sum, v_sum = lax.fori_loop(4, ni, lambda t, s: plane(t - 2, s), carry)

    def share(base, mine, value, group):
        sums[base + mine] = value
        copies = []
        for off, ids in enumerate(group):
            copy = pltpu.make_async_remote_copy(
                src_ref=sums.at[base + mine], dst_ref=sums.at[base + mine],
                send_sem=gsend.at[base + off], recv_sem=grecv.at[base + off],
                device_id=ids, device_id_type=MESH,
            )
            copy.start()
            copies.append(copy)
        return copies

    def gather(base, copies):
        for copy in copies:
            copy.wait()
        total = sums[base]
        for at in range(1, len(copies) + 1):
            total = total + sums[base + at]
        return total

    partial = jnp.concatenate([c_sum[:, :128] + c_sum[:, 128:], v_sum[:, :128] + v_sum[:, 128:]], 0)
    x_sums = share(0, me["gx"], partial, line)
    arrive(x_copies)

    def smooth_x(i, carry):
        lo, hi = carry
        s = 3.0 * wx[i + 2] + 2.0 * (wx[i + 1] + wx[i + 3]) + (wx[i] + wx[i + 4])
        wy[i, 8 : 8 + nj, :] = s
        for at in range(2):
            yslo[at, pl.ds(i, 1), :] = s[at : at + 1]
            yshi[at, pl.ds(i, 1), :] = s[nj - 2 + at : nj - 1 + at]
        mine = (lane >> 1) == i
        lo = jnp.where(mine, pltpu.roll(s[:, 0:128], 2 * i, 1), lo)
        hi = jnp.where(mine, pltpu.roll(s[:, nk - 128 : nk], lax.rem(2 * i + 2, 128), 1), hi)
        return lo, hi

    none = jnp.zeros((nj, 128), F32)
    lo, hi = lax.fori_loop(0, ni, smooth_x, (none, none))
    zslo[...] = lo
    zshi[...] = hi
    side_copies = []
    for at, (b, c) in enumerate(SIDE_STEPS):
        if c:
            rows = (slice(nj - 8, nj), slice(0, nj), slice(0, 8))[1 - b]
            to = (slice(0, 8), slice(8, 8 + nj), slice(8 + nj, 16 + nj))[1 - b]
            src = (zslo if c < 0 else zshi).at[rows]
            dst = rzz.at[1 if c < 0 else 0, to]
        else:
            src, dst = (yslo, ryhi) if b < 0 else (yshi, rylo)
        swap(side_copies, src, dst, fsend.at[at], frecv.at[at], (0, b, c))
    all_sums = share(n["gx"], me["gy"] * nz + me["gz"], gather(0, x_sums), sheet)
    arrive(side_copies)

    def smooth_rows(ref, at):
        return (
            3.0 * ref[at, 8 : 8 + nj, :]
            + 2.0 * (ref[at, 7 : 7 + nj, :] + ref[at, 9 : 9 + nj, :])
            + (ref[at, 6 : 6 + nj, :] + ref[at, 10 : 10 + nj, :])
        )

    for side in range(2):
        packs[side] = smooth_rows(rzz, side)

    def smooth_y(i, carry):
        for at in range(2):
            wy[i, 6 + at : 7 + at, :] = rylo[at, pl.ds(i, 1), :]
            wy[i, 8 + nj + at : 9 + nj + at, :] = ryhi[at, pl.ds(i, 1), :]
        out[i] = smooth_rows(wy, i)
        return carry

    lax.fori_loop(0, ni, smooth_y, 0)
    totals[...] = gather(n["gx"], all_sums)
    for copies in (beside, below, far, x_copies, side_copies):
        finish(copies)


def last_pass(cells, field, packs, totals, out, comp, vol):
    ni, nj, nk = field.shape
    comp[0, 0] = jnp.sum(totals[0:8]) / cells
    vol[0, 0] = jnp.sum(totals[8:16]) / cells
    lanes = iota((nj, nk), 1)

    def twice(x):
        return jnp.concatenate([x, x], 1)

    def smooth_z(i, carry):
        t = field[i]
        left, right = packs[0], packs[1]
        a1 = jnp.where(lanes < 1, twice(pltpu.roll(left, 127 - 2 * i, 1)), pltpu.roll(t, 1, 1))
        a2 = jnp.where(lanes < 2, twice(pltpu.roll(left, lax.rem(128 - 2 * i, 128), 1)), pltpu.roll(t, 2, 1))
        b1 = jnp.where(lanes >= nk - 1, twice(pltpu.roll(right, 127 - 2 * i, 1)), pltpu.roll(t, nk - 1, 1))
        b2 = jnp.where(lanes >= nk - 2, twice(pltpu.roll(right, 126 - 2 * i, 1)), pltpu.roll(t, nk - 2, 1))
        out[i] = 3.0 * t + 2.0 * (a1 + b1) + (a2 + b2)
        return carry

    lax.fori_loop(0, ni, smooth_z, 0)


def on_device(sizes, displacement, density, stiffness):
    ni, nj, nk = density.shape
    vmem = pl.BlockSpec(memory_space=pltpu.VMEM)
    smem = pl.BlockSpec(memory_space=pltpu.SMEM)
    hbm = pl.BlockSpec(memory_space=pltpu.HBM)
    members = sizes[0] + sizes[1] * sizes[2]
    scratch = [
        displacement.shape, density.shape, stiffness.shape,
        (3, nj, nk), (3, ni, nk), (8, nk), (2, 2, nj, 128), (3, ni, nk), (8, nk), (nj, 128),
        (2, 3, ni + 1, nj + 8, nk),
    ]
    later = [
        (ni + 4, nj, nk), (ni, nj + 16, nk),
        (2, ni, nk), (2, ni, nk), (2, ni, nk), (2, ni, nk),
        (nj, 128), (nj, 128), (2, nj + 16, 128), (members, 16, 128),
    ]
    field, packs, totals = pl.pallas_call(
        functools.partial(kernel, sizes),
        out_shape=(
            jax.ShapeDtypeStruct((ni, nj, nk), F32),
            jax.ShapeDtypeStruct((2, nj, 128), F32),
            jax.ShapeDtypeStruct((16, 128), F32),
        ),
        in_specs=[hbm] * 3,
        out_specs=(vmem, vmem, vmem),
        scratch_shapes=[pltpu.VMEM(shape, F32) for shape in scratch]
        + [pltpu.VMEM((nj // 8, (ni + 1) * 128, nk), BF16), pltpu.VMEM((384, 256), BF16)]
        + [pltpu.VMEM(shape, F32) for shape in later]
        + [pltpu.SemaphoreType.DMA((count,)) for count in (3, 7, 7, 10, 10, members, members)],
        compiler_params=pltpu.CompilerParams(
            collective_id=0, has_side_effects=True, vmem_limit_bytes=24 * 1024 * 1024
        ),
    )(*(pltpu.with_memory_space_constraint(x, pltpu.HBM) for x in (displacement, density, stiffness)))
    cells = float(ni * nj * nk * sizes[0] * sizes[1] * sizes[2])
    filtered, comp, vol = pl.pallas_call(
        functools.partial(last_pass, cells),
        out_shape=(
            jax.ShapeDtypeStruct((ni, nj, nk), F32),
            jax.ShapeDtypeStruct((1, 1), F32),
            jax.ShapeDtypeStruct((1, 1), F32),
        ),
        in_specs=[vmem] * 3,
        out_specs=(vmem, smem, smem),
        compiler_params=pltpu.CompilerParams(vmem_limit_bytes=24 * 1024 * 1024),
    )(field, packs, totals)
    return filtered, comp.reshape(()), vol.reshape(())


def solution(mesh):
    sizes = tuple(mesh.shape[axis] for axis in AXES)
    return jax.shard_map(
        functools.partial(on_device, sizes),
        mesh=mesh,
        in_specs=(P(None, "gx", "gy", "gz"), P("gx", "gy", "gz"), P()),
        out_specs=(P("gx", "gy", "gz"), P(), P()),
        check_vma=False,
    )
```

```python
import functools

import jax
import jax.numpy as jnp
from jax import lax
from jax.experimental import pallas as pl
from jax.experimental.pallas import tpu as pltpu
from jax.sharding import PartitionSpec as P

VOID = 0.001
H = (1.0, 2.0, 3.0, 2.0, 1.0)
MESH = pl.DeviceIdType.MESH
AXES = ("gx", "gy", "gz")
F32 = jnp.float32
BF16 = jnp.bfloat16
NODE_STEPS = [(a, b, c) for a in (0, 1) for b in (0, 1) for c in (0, 1) if a + b + c]
SIDE_STEPS = [(b, c) for b in (-1, 0, 1) for c in (-1, 0, 1) if b or c]


def iota(shape, dim):
    return lax.broadcasted_iota(jnp.int32, shape, dim)


def line_sum(position, extent):
    total = None
    for d in range(5):
        at = position + (d - 2)
        term = jnp.where((at >= 0) & (at < extent), H[d], 0.0).astype(F32)
        total = term if total is None else total + term
    return total


def band_weights(stiff):
    rows, cols = 192, 256
    pick = jnp.where((iota((rows, 24), 0) >> 3) == iota((rows, 24), 1), 1.0, 0.0).astype(F32)

    def column(shape):
        col = iota(shape, 1)
        a, g, s = col >> 7, (col >> 4) & 7, col & 7
        cm = jnp.where(g == 6, s, g)
        c = jnp.where(cm >= 3, 1, 0)
        m = cm - 3 * c
        valid = (g < 6) | ((g == 6) & (s < 6))
        return 8 * m + 4 * a + c, valid, jnp.where(g == 6, 8, s), (col >> 3) & 1

    total = None
    for b in (0, 1):
        q, valid, _, _ = column((24, cols))
        place = jnp.where((iota((24, cols), 0) == q + 2 * b) & valid, 1.0, 0.0).astype(F32)
        wide = jnp.dot(stiff, place, precision=lax.Precision.HIGHEST, preferred_element_type=F32)
        tall = jnp.dot(pick, wide, precision=lax.Precision.HIGHEST, preferred_element_type=F32)
        _, _, jj, _ = column((rows, cols))
        term = jnp.where(jj - (iota((rows, cols), 0) & 7) == b, tall, 0.0)
        total = term if total is None else total + term
    high = total.astype(BF16).astype(F32)
    _, _, _, lo_col = column((rows, cols))
    low = jnp.where(lo_col == 0, total - high, 0.0)
    return high.astype(BF16), low.astype(BF16)


def kernel(
    sizes, u_hbm, rho_hbm, stiff_hbm, out, packs, totals,
    u, rho, stiff, rx, ry, rxy, rz, ys, yd, zs, field, parts, weights, wx, wy,
    yslo, yshi, rylo, ryhi, zslo, zshi, rzz, sums, insem, nsend, nrecv, fsend, frecv, gsend, grecv,
):
    ni, nj, nk = rho.shape
    n = dict(zip(AXES, sizes))
    me = {axis: lax.axis_index(axis) for axis in AXES}
    ny, nz = n["gy"], n["gz"]
    down = {axis: me[axis] > 0 for axis in AXES}
    up = {axis: me[axis] < n[axis] - 1 for axis in AXES}

    loads = []
    for at, (src, dst) in enumerate(((stiff_hbm, stiff), (u_hbm, u), (rho_hbm, rho))):
        copy = pltpu.make_async_copy(src, dst, insem.at[at])
        copy.start()
        loads.append(copy)

    def hop(step):
        ids, ok = {}, None
        for axis, s in zip(AXES, step):
            if s:
                ids[axis] = me[axis] + s
                flag = up[axis] if s > 0 else down[axis]
                ok = flag if ok is None else jnp.logical_and(ok, flag)
        return ids, ok

    def minus(step):
        return tuple(-s for s in step)

    line = [{"gx": lax.rem(me["gx"] + off, n["gx"])} for off in range(1, n["gx"])]
    sheet = [
        {"gy": lax.rem(me["gy"] + off // nz, ny), "gz": lax.rem(me["gz"] + off % nz, nz)}
        for off in range(1, ny * nz)
    ]
    barrier = pltpu.get_barrier_semaphore()
    for ids in line + sheet:
        pl.semaphore_signal(barrier, inc=1, device_id=ids, device_id_type=MESH)
    peers = len(line) + len(sheet)
    for step in NODE_STEPS:
        if step[0] and sum(step) > 1:
            for way in (step, minus(step)):
                ids, ok = hop(way)
                peers = peers + jnp.where(ok, 1, 0)

                @pl.when(ok)
                def _():
                    pl.semaphore_signal(barrier, inc=1, device_id=ids, device_id_type=MESH)

    pl.semaphore_wait(barrier, peers)

    def swap(copies, src, dst, send_sem, recv_sem, step):
        ids, sends = hop(step)
        copy = pltpu.make_async_remote_copy(
            src_ref=src, dst_ref=dst, send_sem=send_sem, recv_sem=recv_sem,
            device_id=ids, device_id_type=MESH,
        )
        copies.append((copy, sends, hop(minus(step))[1], dst))

        @pl.when(sends)
        def _():
            copy.start()

    def arrive(copies):
        for copy, _, takes, dst in copies:

            @pl.when(takes)
            def _():
                copy.wait_recv()

            @pl.when(jnp.logical_not(takes))
            def _():
                dst[...] = jnp.zeros(dst.shape, F32)

    def finish(copies):
        for copy, sends, _, _ in copies:

            @pl.when(sends)
            def _():
                copy.wait_send()

    beside, below, far = [], [], []

    def node_swap(step):
        a, b, c = step
        at = NODE_STEPS.index(step)
        if c:
            src, dst = (zs.at[0:8], rz.at[a, b, 0:8]) if b else (zs, rz.at[a, b])
        elif b:
            src, dst = (yd, rxy) if a else (ys, ry)
        else:
            src, dst = u_hbm.at[:, 0], rx
        copies = far if a else (below if b else beside)
        swap(copies, src, dst, nsend.at[at], nrecv.at[at], minus(step))

    node_swap((1, 0, 0))
    loads[1].wait()
    lane = iota((nj, 128), 1)
    def pack(i, acc):
        for m in range(3):
            at = m * ni + i
            acc = jnp.where(lane == at, pltpu.roll(u[m, i, :, 0:128], at, 1), acc)
        return acc

    zs[...] = lax.fori_loop(0, ni, pack, jnp.zeros((nj, 128), F32), unroll=4)
    for step in NODE_STEPS:
        if step[2]:
            node_swap(step)
    yd[...] = jnp.zeros(yd.shape, F32)
    for m in range(3):
        for i in range(ni):
            ys[m, i : i + 1, :] = u[m, i, 0:1, :]
        yd[m : m + 1, :] = u[m, 0, 0:1, :]
    node_swap((0, 1, 0))
    node_swap((1, 1, 0))
    loads[0].wait()
    high, low = band_weights(stiff[...])
    weights[0:192, :] = high
    weights[192:384, :] = low

    last = iota((nj, nk), 1) == nk - 1
    last8 = iota((8, nk), 1) == nk - 1
    sub8 = iota((8, nk), 0)

    def split(f):
        hi = f.astype(BF16).astype(F32)
        return jnp.concatenate([hi, f - hi], 0).astype(BF16)

    def put(jt, to, at, f):
        parts[jt, pl.ds(pl.multiple_of(to * 128, 128) + at, 16), :] = split(f)

    def first_half(m, to, base):
        field[0, m, to, 0:nj, :] = base
        for jt in range(nj // 8):
            put(jt, to, 16 * m, base[8 * jt : 8 * jt + 8])

    def second_half(m, to, base, col, at):
        side = pltpu.roll(col, 127 - at, 1)
        moved = jnp.where(last, jnp.concatenate([side, side], 1), pltpu.roll(base, nk - 1, 1))
        field[1, m, to, 0:nj, :] = moved
        for jt in range(nj // 8):
            put(jt, to, 48 + 16 * m, moved[8 * jt : 8 * jt + 8])

    def next_row(m, to, row, corner, at):
        row8 = jnp.broadcast_to(row, (8, nk))
        field[0, m, to, nj : nj + 8, :] = row8
        side8 = pltpu.roll(corner, 127 - at, 1)
        field[1, m, to, nj : nj + 8, :] = jnp.where(
            last8, jnp.concatenate([side8, side8], 1), pltpu.roll(row8, nk - 1, 1)
        )

    def edges(to):
        for jt in range(nj // 8):
            edge = jnp.zeros((8, nk), F32)
            for cm in range(6):
                c, m = divmod(cm, 3)
                row = field[c, m, to, 8 * jt + 8 : 8 * jt + 9, :]
                edge = jnp.where(sub8 == cm, jnp.broadcast_to(row, (8, nk)), edge)
            put(jt, to, 96, edge)

    def own_first(i, carry):
        for m in range(3):
            first_half(m, i, u[m, i])
        for jt in range(nj // 8):
            parts[jt, pl.ds(pl.multiple_of(i * 128, 128) + 112, 16), :] = jnp.zeros((16, nk), BF16)
        return carry

    def own_second(i, carry):
        for m in range(3):
            second_half(m, i, u[m, i], rz[0, 0], m * ni + i)
        return carry

    def own_edges(i, carry):
        for m in range(3):
            next_row(m, i, ry[m, pl.ds(i, 1), :], rz[0, 1, 0:8, :], m * ni + i)
        edges(i)
        return carry

    lax.fori_loop(0, ni, own_first, 0)
    for jt in range(nj // 8):
        parts[jt, ni * 128 + 112 : ni * 128 + 128, :] = jnp.zeros((16, nk), BF16)
    loads[2].wait()
    wy[0, 0:nj, :] = 1.0 / (
        line_sum(me["gy"] * nj + iota((nj, nk), 0), ny * nj)
        * line_sum(me["gz"] * nk + iota((nj, nk), 1), nz * nk)
    )
    arrive(beside)
    lax.fori_loop(0, ni, own_second, 0, unroll=2)
    arrive(below)
    lax.fori_loop(0, ni, own_edges, 0, unroll=2)
    arrive(far)
    for m in range(3):
        first_half(m, ni, rx[m])
        second_half(m, ni, rx[m], rz[1, 0], m * ni)
        next_row(m, ni, rxy[m : m + 1, :], rz[1, 1, 0:8, :], m * ni)
    edges(ni)

    def plane(i, carry):
        c_sum, v_sum = carry
        inv_x = 1.0 / line_sum(jnp.full((8, nk), me["gx"] * ni + i, jnp.int32), n["gx"] * ni)
        for jt in range(nj // 8):
            data = parts[jt, pl.ds(pl.multiple_of(i * 128, 128), 256), :]
            product = jnp.dot(weights[...], data, preferred_element_type=F32)
            energy = None
            for r in range(24):
                m, a, b, c = r >> 3, (r >> 2) & 1, (r >> 1) & 1, r & 1
                v = product[8 * r : 8 * r + 8] + product[192 + 8 * r : 200 + 8 * r]
                term = v * field[c, m, i + a, 8 * jt + b : 8 * jt + b + 8, :]
                energy = term if energy is None else energy + term
            d = rho[i, 8 * jt : 8 * jt + 8, :]
            c_sum = c_sum + (VOID + d * d * d * (1.0 - VOID)) * energy
            v_sum = v_sum + d
            wx[i + 2, 8 * jt : 8 * jt + 8, :] = (
                (-3.0 * (1.0 - VOID)) * d * d * energy * (inv_x * wy[0, 8 * jt : 8 * jt + 8, :])
            )
        return c_sum, v_sum

    zero = jnp.zeros((8, nk), F32)
    carry = lax.fori_loop(
        0, 4, lambda t, s: plane(jnp.where(t < 2, t, ni - 4 + t), s), (zero, zero)
    )
    x_copies = []
    swap(x_copies, wx.at[2:4], wx.at[ni + 2 : ni + 4], fsend.at[8], frecv.at[8], (-1, 0, 0))
    swap(x_copies, wx.at[ni : ni + 2], wx.at[0:2], fsend.at[9], frecv.at[9], (1, 0, 0))
    c_sum, v_sum = lax.fori_loop(4, ni, lambda t, s: plane(t - 2, s), carry)

    def share(base, mine, value, group):
        sums[base + mine] = value
        copies = []
        for off, ids in enumerate(group):
            copy = pltpu.make_async_remote_copy(
                src_ref=sums.at[base + mine], dst_ref=sums.at[base + mine],
                send_sem=gsend.at[base + off], recv_sem=grecv.at[base + off],
                device_id=ids, device_id_type=MESH,
            )
            copy.start()
            copies.append(copy)
        return copies

    def gather(base, copies):
        for copy in copies:
            copy.wait()
        total = sums[base]
        for at in range(1, len(copies) + 1):
            total = total + sums[base + at]
        return total


    def fold(x):
        row = jnp.sum(x, axis=0, keepdims=True)
        row = row[:, :128] + row[:, 128:]
        return row + pltpu.roll(row, 64, 1)

    partial = jnp.where(iota((1, 128), 1) < 64, fold(c_sum), fold(v_sum))
    x_sums = share(0, me["gx"], partial, line)
    arrive(x_copies)

    def smooth_x(i, carry):
        lo, hi = carry
        s = 3.0 * wx[i + 2] + 2.0 * (wx[i + 1] + wx[i + 3]) + (wx[i] + wx[i + 4])
        wy[i, 8 : 8 + nj, :] = s
        for at in range(2):
            yslo[at, pl.ds(i, 1), :] = s[at : at + 1]
            yshi[at, pl.ds(i, 1), :] = s[nj - 2 + at : nj - 1 + at]
        mine = (lane >> 1) == i
        lo = jnp.where(mine, pltpu.roll(s[:, 0:128], 2 * i, 1), lo)
        hi = jnp.where(mine, pltpu.roll(s[:, nk - 128 : nk], lax.rem(2 * i + 2, 128), 1), hi)
        return lo, hi

    none = jnp.zeros((nj, 128), F32)
    lo, hi = lax.fori_loop(0, ni, smooth_x, (none, none), unroll=4)
    zslo[...] = lo
    zshi[...] = hi
    side_copies = []
    for at, (b, c) in enumerate(SIDE_STEPS):
        if c:
            rows = (slice(nj - 8, nj), slice(0, nj), slice(0, 8))[1 - b]
            to = (slice(0, 8), slice(8, 8 + nj), slice(8 + nj, 16 + nj))[1 - b]
            src = (zslo if c < 0 else zshi).at[rows]
            dst = rzz.at[1 if c < 0 else 0, to]
        else:
            src, dst = (yslo, ryhi) if b < 0 else (yshi, rylo)
        swap(side_copies, src, dst, fsend.at[at], frecv.at[at], (0, b, c))
    all_sums = share(n["gx"], me["gy"] * nz + me["gz"], gather(0, x_sums), sheet)
    arrive(side_copies)

    def smooth_rows(ref, at):
        return (
            3.0 * ref[at, 8 : 8 + nj, :]
            + 2.0 * (ref[at, 7 : 7 + nj, :] + ref[at, 9 : 9 + nj, :])
            + (ref[at, 6 : 6 + nj, :] + ref[at, 10 : 10 + nj, :])
        )

    for side in range(2):
        packs[side] = smooth_rows(rzz, side)

    def smooth_y(i, carry):
        for at in range(2):
            wy[i, 6 + at : 7 + at, :] = rylo[at, pl.ds(i, 1), :]
            wy[i, 8 + nj + at : 9 + nj + at, :] = ryhi[at, pl.ds(i, 1), :]
        out[i] = smooth_rows(wy, i)
        return carry

    lax.fori_loop(0, ni, smooth_y, 0, unroll=4)
    totals[...] = gather(n["gx"], all_sums)
    for copies in (beside, below, far, x_copies, side_copies):
        finish(copies)


def last_pass(cells, field, packs, totals, out, comp, vol):
    ni, nj, nk = field.shape
    both = totals[...]
    first = iota((1, 128), 1) < 64
    comp[0, 0] = jnp.sum(jnp.where(first, both, 0.0)) / cells
    vol[0, 0] = jnp.sum(jnp.where(first, 0.0, both)) / cells
    lanes = iota((nj, nk), 1)

    def twice(x):
        return jnp.concatenate([x, x], 1)

    def smooth_z(i, carry):
        t = field[i]
        left, right = packs[0], packs[1]
        a1 = jnp.where(lanes < 1, twice(pltpu.roll(left, 127 - 2 * i, 1)), pltpu.roll(t, 1, 1))
        a2 = jnp.where(lanes < 2, twice(pltpu.roll(left, lax.rem(128 - 2 * i, 128), 1)), pltpu.roll(t, 2, 1))
        b1 = jnp.where(lanes >= nk - 1, twice(pltpu.roll(right, 127 - 2 * i, 1)), pltpu.roll(t, nk - 1, 1))
        b2 = jnp.where(lanes >= nk - 2, twice(pltpu.roll(right, 126 - 2 * i, 1)), pltpu.roll(t, nk - 2, 1))
        out[i] = 3.0 * t + 2.0 * (a1 + b1) + (a2 + b2)
        return carry

    lax.fori_loop(0, ni, smooth_z, 0, unroll=4)


def on_device(sizes, displacement, density, stiffness):
    ni, nj, nk = density.shape
    vmem = pl.BlockSpec(memory_space=pltpu.VMEM)
    smem = pl.BlockSpec(memory_space=pltpu.SMEM)
    hbm = pl.BlockSpec(memory_space=pltpu.HBM)
    members = sizes[0] + sizes[1] * sizes[2]
    scratch = [
        displacement.shape, density.shape, stiffness.shape,
        (3, nj, nk), (3, ni, nk), (8, nk), (2, 2, nj, 128), (3, ni, nk), (8, nk), (nj, 128),
        (2, 3, ni + 1, nj + 8, nk),
    ]
    later = [
        (ni + 4, nj, nk), (ni, nj + 16, nk),
        (2, ni, nk), (2, ni, nk), (2, ni, nk), (2, ni, nk),
        (nj, 128), (nj, 128), (2, nj + 16, 128), (members, 1, 128),
    ]
    field, packs, totals = pl.pallas_call(
        functools.partial(kernel, sizes),
        out_shape=(
            jax.ShapeDtypeStruct((ni, nj, nk), F32),
            jax.ShapeDtypeStruct((2, nj, 128), F32),
            jax.ShapeDtypeStruct((1, 128), F32),
        ),
        in_specs=[hbm] * 3,
        out_specs=(vmem, vmem, vmem),
        scratch_shapes=[pltpu.VMEM(shape, F32) for shape in scratch]
        + [pltpu.VMEM((nj // 8, (ni + 1) * 128, nk), BF16), pltpu.VMEM((384, 256), BF16)]
        + [pltpu.VMEM(shape, F32) for shape in later]
        + [pltpu.SemaphoreType.DMA((count,)) for count in (3, 7, 7, 10, 10, members, members)],
        compiler_params=pltpu.CompilerParams(
            collective_id=0, has_side_effects=True, vmem_limit_bytes=24 * 1024 * 1024
        ),
    )(*(pltpu.with_memory_space_constraint(x, pltpu.HBM) for x in (displacement, density, stiffness)))
    cells = float(ni * nj * nk * sizes[0] * sizes[1] * sizes[2])
    filtered, comp, vol = pl.pallas_call(
        functools.partial(last_pass, cells),
        out_shape=(
            jax.ShapeDtypeStruct((ni, nj, nk), F32),
            jax.ShapeDtypeStruct((1, 1), F32),
            jax.ShapeDtypeStruct((1, 1), F32),
        ),
        in_specs=[vmem] * 3,
        out_specs=(vmem, smem, smem),
        compiler_params=pltpu.CompilerParams(vmem_limit_bytes=24 * 1024 * 1024),
    )(field, packs, totals)
    return filtered, comp.reshape(()), vol.reshape(())


def solution(mesh):
    sizes = tuple(mesh.shape[axis] for axis in AXES)
    return jax.shard_map(
        functools.partial(on_device, sizes),
        mesh=mesh,
        in_specs=(P(None, "gx", "gy", "gz"), P("gx", "gy", "gz"), P()),
        out_specs=(P("gx", "gy", "gz"), P(), P()),
        check_vma=False,
    )
```
